32 devices in a mesh: row: 16 (over z, y, x), col: 2 (over core).
Axes of the slice: x: 2, y: 2, z: 4, core: 2. Of those that a mesh axis runs over, the one named last changes fastest.
Arguments:
- tokens: bfloat16 [256, 8192], P('row', 'col'), may hold values from -6 to 6
- norm_gain: float32 [8192], P('col'), may hold values from 0.1 to 1.9
- gate_weight: bfloat16 [8192, 28672], P('col', 'row'), may hold values from -0.0625 to 0.0625
- up_weight: bfloat16 [8192, 28672], P('col', 'row'), may hold values from -0.0625 to 0.0625
- down_weight: bfloat16 [28672, 8192], P('row', 'col'), may hold values from -0.03125 to 0.03125
Outputs:
- mixed: bfloat16 [256, 8192], P('row', 'col')
The draws below stay inside these ranges and needn't reach their ends.
All inputs are finite; a program needn't handle non-finite values.
Results may differ from the reference program's by a relative error of at most 0.0065.
Values may be sent and summed in bfloat16 or wider, within the bound.
A program may use at most 128 MiB of HBM per device.

```python
import jax
import jax.numpy as jnp
from jax import lax

D = 8192
FF = 28672
TOKENS = 256


def block_levels(rng, dims, shards, smallest, largest):
    def one(position, parts):
        heights = jax.random.uniform(jax.random.fold_in(jax.random.fold_in(rng, 6), position), (parts,), jnp.float32, smallest / len(shards), largest / len(shards))
        return jnp.repeat(jnp.exp(heights), dims[position] // parts).reshape((-1,) + (1,) * (len(dims) - position - 1))

    level = one(*shards[0])
    for cut in shards[1:]:
        level = level * one(*cut)
    return level


def centred(stream_key, extent, deviation, reach, cuts=(), held_as=jnp.bfloat16):
    array = jax.random.normal(stream_key, extent, jnp.float32) * deviation
    if len(cuts) > 0:
        array = block_levels(stream_key, extent, cuts, -0.22, 0.18) * array
    return jnp.clip(array, min=-reach, max=reach).astype(held_as)


def setup_inputs(seed: int = 0) -> dict:
    seeds = jax.random.split(jax.random.key(seed), 6)
    tokens = centred(seeds[0], (TOKENS, D), 1.0, 6.0, ((0, 16), (1, 2)))
    norm_gain = jnp.clip(1.0 + 0.18 * jax.random.normal(seeds[1], (D,), jnp.float32), 0.1, 1.9)
    gate_weight = centred(seeds[2], (D, FF), D ** -0.5, 0.0625, ((0, 2), (1, 16)))
    up_weight = centred(seeds[3], (D, FF), D ** -0.5, 0.0625, ((0, 2), (1, 16)))
    down_weight = centred(seeds[4], (FF, D), FF ** -0.5, 0.03125, ((0, 16), (1, 2)))
    return dict(tokens=tokens, norm_gain=norm_gain, gate_weight=gate_weight, up_weight=up_weight, down_weight=down_weight)


def reference(tokens, norm_gain, gate_weight, up_weight, down_weight):
    widened = tokens.astype(jnp.float32)
    squares = lax.optimization_barrier(jnp.sum(widened * widened, axis=1, keepdims=True))
    normed = (widened * norm_gain[None, :] / jnp.sqrt(squares / D + 1e-05)).astype(jnp.bfloat16)
    gate = jnp.dot(normed, gate_weight, preferred_element_type=jnp.float32)
    up = jnp.dot(normed, up_weight, preferred_element_type=jnp.float32)
    hidden = (jax.nn.silu(gate) * up).astype(jnp.bfloat16)
    return jnp.dot(hidden, down_weight, preferred_element_type=jnp.float32).astype(jnp.bfloat16)
```

```python
import functools

import jax
import jax.numpy as jnp
from jax import lax
from jax.experimental import pallas as pl
from jax.experimental.pallas import tpu as pltpu
from jax.sharding import PartitionSpec as P

MESH = pl.DeviceIdType.MESH
D = 8192
F32 = jnp.float32
BF16 = jnp.bfloat16


def tile_of(width):
    return 256 if width % 256 == 0 else width


def kernel(line, rounds, tokens, gain, gate_hbm, up_hbm, down_hbm, out,
           wg, wu, wd, act, gacc, uacc, rg, ru, hid, part, xa, yb, ya, xb, sa, sb, vs, zin, own, sq,
           wsem, sqs, ag_send, ag_z, ag_x, ag_y, ag_xh, ag_yh, c_send, cg, cu, ch,
           rs_s, rs_r, rz_s, rz_r):
    tb, dc = tokens.shape
    ff = wg.shape[1]
    n = 4 * line
    total = n * tb
    wide = dc // rounds
    half = wide // 2
    me = lax.axis_index("row")
    c = lax.axis_index("col")
    l, j, i = me // 4, (me // 2) % 2, me % 2

    def row(a, b, d):
        return (a * 2 + b) * 2 + d

    x_id = {"row": row(l, j, 1 - i)}
    y_id = {"row": row(l, 1 - j, i)}
    p_id = {"col": 1 - c}

    def z_at(k):
        return lax.rem(l + k, line)

    def from_z(k):
        return lax.rem(l + line - k, line)

    def z_id(k):
        return {"row": row(z_at(k), j, i)}

    def remote(src, dst, ssem, rsem, dev):
        return pltpu.make_async_remote_copy(src_ref=src, dst_ref=dst, send_sem=ssem, recv_sem=rsem,
                                            device_id=dev, device_id_type=MESH)

    loads = []
    for r in range(rounds):
        rows = pl.ds(r * wide, wide)
        loads.append([pltpu.make_async_copy(gate_hbm.at[rows], wg.at[rows], wsem.at[3 * r]),
                      pltpu.make_async_copy(up_hbm.at[rows], wu.at[rows], wsem.at[3 * r + 1])])
    frows = ff // rounds
    downs = [pltpu.make_async_copy(down_hbm.at[pl.ds(r * frows, frows)], wd.at[pl.ds(r * frows, frows)],
                                   wsem.at[3 * r + 2]) for r in range(rounds)]
    for pair in loads:
        for d in pair:
            d.start()
    for d in downs:
        d.start()

    barrier = pltpu.get_barrier_semaphore()
    friends = [x_id, y_id, p_id] + [z_id(k) for k in range(1, line)]
    for dev in friends:
        pl.semaphore_signal(barrier, inc=1, device_id=dev, device_id_type=MESH)

    widened = tokens[...].astype(F32)
    mine = jnp.sum(widened * widened, axis=1, keepdims=True)
    sq[0] = jnp.broadcast_to(mine, (tb, 128))
    pl.semaphore_wait(barrier, len(friends))
    swap = remote(sq.at[0], sq.at[1], sqs.at[0], sqs.at[1], p_id)
    swap.start()
    scaled = widened * gain[...]
    swap.wait()
    squares = mine + sq[1][:, :1]
    act[me] = (scaled / jnp.sqrt(squares / D + 1e-05)).astype(BF16)

    def cols(r):
        return pl.ds(r * wide, wide)

    def cols_a(r):
        return pl.ds(r * wide, half)

    def cols_b(r):
        return pl.ds(r * wide + half, half)

    def move(b, where, sem, ssem, dev):
        ref = act.at[b, :, where]
        return remote(ref, ref, ssem, sem, dev)

    def to_xy(r, k):
        b = row(from_z(k), j, i)
        move(b, cols(r), ag_x.at[r * line + k], ag_send.at[0], x_id).start()
        move(b, cols(r), ag_y.at[r * line + k], ag_send.at[1], y_id).start()

    for r in range(rounds):
        for k in range(1, line):
            move(me, cols(r), ag_z.at[r * line + k], ag_send.at[2], z_id(k)).start()
        to_xy(r, 0)

    def forward(r):
        for k in range(1, line):
            move(row(from_z(k), j, i), cols(r), ag_z.at[r * line + k], ag_send.at[2], z_id(k)).wait_recv()
            to_xy(r, k)
        for k in range(line):
            b = row(from_z(k), 1 - j, i)
            move(b, cols(r), ag_y.at[r * line + k], ag_send.at[1], y_id).wait_recv()
            move(b, cols_a(r), ag_xh.at[r * line + k], ag_send.at[0], x_id).start()
            b = row(from_z(k), j, 1 - i)
            move(b, cols(r), ag_x.at[r * line + k], ag_send.at[0], x_id).wait_recv()
            move(b, cols_b(r), ag_yh.at[r * line + k], ag_send.at[1], y_id).start()

    def last_arrivals(r):
        for k in range(line):
            b = row(from_z(k), 1 - j, 1 - i)
            move(b, cols_a(r), ag_xh.at[r * line + k], ag_send.at[0], x_id).wait_recv()
            move(b, cols_b(r), ag_yh.at[r * line + k], ag_send.at[1], y_id).wait_recv()

    tw = tile_of(ff)
    tiles = ff // tw
    mrows = total // 2

    def tile(t):
        return pl.ds(pl.multiple_of(t * tw, tw), tw) if tiles > 1 else pl.ds(0, tw)

    theirs = pl.ds(pl.multiple_of((1 - c) * mrows, mrows), mrows)
    ours = pl.ds(pl.multiple_of(c * mrows, mrows), mrows)
    mstep = min(total, 256)

    def swap_tile(t):
        return [remote(gacc.at[theirs, tile(t)], rg.at[:, tile(t)], c_send.at[0], cg.at[t], p_id),
                remote(uacc.at[theirs, tile(t)], ru.at[:, tile(t)], c_send.at[1], cu.at[t], p_id)]

    def project(r):
        for d in loads[r]:
            d.wait()
        wrows = pl.ds(r * wide, wide)
        last = r == rounds - 1

        def body(t, carry):
            for m in range(0, total, mstep):
                left = act[m // tb:(m + mstep) // tb, :, r * wide:(r + 1) * wide].reshape(mstep, wide)
                at = pl.ds(m, mstep)
                for w, acc in ((wg, gacc), (wu, uacc)):
                    value = jnp.dot(left, w[wrows, tile(t)], preferred_element_type=F32)
                    if r > 0:
                        value = acc[at, tile(t)] + value
                    acc[at, tile(t)] = value
            if last:
                @pl.when(t > 0)
                def _():
                    for d in swap_tile(t - 1):
                        d.start()
            return carry

        lax.fori_loop(0, tiles, body, 0)
        if last:
            for d in swap_tile(tiles - 1):
                d.start()

    forward(0)
    for r in range(rounds):
        if r + 1 < rounds:
            forward(r + 1)
        last_arrivals(r)
        project(r)

    def hid_tile(t):
        ref = hid.at[ours, tile(t)]
        return remote(ref, ref, c_send.at[2], ch.at[t], p_id)

    def gated(t, carry):
        for d in swap_tile(t):
            d.wait_recv()
        g = gacc[ours, tile(t)] + rg[:, tile(t)]
        u = uacc[ours, tile(t)] + ru[:, tile(t)]
        hid[ours, tile(t)] = (g / (1.0 + jnp.exp(-g)) * u).astype(BF16)

        @pl.when(t > 0)
        def _():
            hid_tile(t - 1).start()
        return carry

    lax.fori_loop(0, tiles, gated, 0)
    hid_tile(tiles - 1).start()
    for d in downs:
        d.wait()
    for t in range(tiles):
        ref = hid.at[theirs, tile(t)]
        remote(ref, ref, c_send.at[2], ch.at[t], p_id).wait_recv()

    ow = tile_of(wide)
    oblocks = mstep // (4 * tb)

    def down(r):
        def body(t, carry):
            at = pl.ds(pl.multiple_of(r * wide + t * ow, ow), ow)
            for m in range(0, total, mstep):
                value = jnp.dot(hid[pl.ds(m, mstep), :], wd[:, at], preferred_element_type=F32)
                first = m // (4 * tb)
                part[first:first + oblocks, :, :, :, at] = value.astype(BF16).reshape(oblocks, 2, 2, tb, ow)
            return carry

        lax.fori_loop(0, wide // ow, body, 0)

    def first_x(r):
        return remote(part.at[:, :, 1 - i, :, cols_a(r)], xa.at[r], rs_s.at[4 * r], rs_r.at[4 * r], x_id)

    def first_y(r):
        return remote(part.at[:, 1 - j, :, :, cols_b(r)], yb.at[r], rs_s.at[4 * r + 1], rs_r.at[4 * r + 1], y_id)

    def second_y(r):
        return remote(sa.at[r], ya.at[r], rs_s.at[4 * r + 2], rs_r.at[4 * r + 2], y_id)

    def second_x(r):
        return remote(sb.at[r], xb.at[r], rs_s.at[4 * r + 3], rs_r.at[4 * r + 3], x_id)

    def third(r, k):
        return remote(vs.at[r, z_at(k)], zin.at[r, k], rz_s.at[r * line + k], rz_r.at[r * line + k], z_id(k))

    def s1(r):
        first_x(r).start()
        first_y(r).start()

    def s2(r):
        first_x(r).wait_recv()
        sa[r] = (part[:, 1 - j, i, :, cols_a(r)].astype(F32) + xa[r, :, 1 - j].astype(F32)).astype(BF16)
        first_y(r).wait_recv()
        sb[r] = (part[:, j, 1 - i, :, cols_b(r)].astype(F32) + yb[r, :, 1 - i].astype(F32)).astype(BF16)
        second_y(r).start()
        second_x(r).start()

    def s3(r):
        second_y(r).wait_recv()
        second_x(r).wait_recv()
        for where, near, far, lo in ((cols_a(r), xa, ya, 0), (cols_b(r), yb, xb, half)):
            mid = j if lo == 0 else i
            vs[r, :, :, lo:lo + half] = (part[:, j, i, :, where].astype(F32) + near[r, :, mid].astype(F32)
                                         + far[r].astype(F32)).astype(BF16)
            own[:, where] = (part[l, j, i, :, where].astype(F32) + near[r, l, mid].astype(F32)
                             + far[r, l].astype(F32))
        for k in range(1, line):
            third(r, k).start()

    def s4(r):
        value = own[:, cols(r)]
        for k in range(1, line):
            third(r, k).wait_recv()
            value = value + zin[r, k].astype(F32)
        out[:, cols(r)] = value.astype(BF16)

    for r in range(rounds):
        down(r)
        if r < 2:
            s1(r)
    for r in range(rounds + 2):
        if r < rounds:
            s2(r)
            if r + 2 < rounds:
                s1(r + 2)
        if 1 <= r <= rounds:
            s3(r - 1)
        if r >= 2:
            s4(r - 2)

    for s, count in ((0, 3 * line // 2), (1, 3 * line // 2), (2, line - 1)):
        ref = act.at[pl.ds(0, count)]
        remote(ref, ref, ag_send.at[s], ag_z.at[0], x_id).wait_send()
    remote(rg, rg, c_send.at[0], cg.at[0], p_id).wait_send()
    remote(ru, ru, c_send.at[1], cu.at[0], p_id).wait_send()
    ref = hid.at[pl.ds(0, mrows)]
    remote(ref, ref, c_send.at[2], ch.at[0], p_id).wait_send()
    for r in range(rounds):
        for make in (first_x, first_y, second_x, second_y):
            make(r).wait_send()
        for k in range(1, line):
            third(r, k).wait_send()


def solution(mesh):
    n = mesh.shape["row"]
    line = n // 4

    def step(tokens, norm_gain, gate_weight, up_weight, down_weight):
        tb, dc = tokens.shape
        ff = gate_weight.shape[1]
        total = n * tb
        rounds = 4
        half = dc // rounds // 2
        tiles = ff // tile_of(ff)
        dma = pltpu.SemaphoreType.DMA
        vmem = pl.BlockSpec(memory_space=pltpu.VMEM)
        hbm = pl.BlockSpec(memory_space=pl.ANY)
        return pl.pallas_call(
            functools.partial(kernel, line, rounds),
            out_shape=jax.ShapeDtypeStruct((tb, dc), BF16),
            in_specs=[vmem, vmem, hbm, hbm, hbm],
            out_specs=vmem,
            scratch_shapes=[
                pltpu.VMEM((dc, ff), BF16),
                pltpu.VMEM((dc, ff), BF16),
                pltpu.VMEM((ff, dc), BF16),
                pltpu.VMEM((n, tb, dc), BF16),
                pltpu.VMEM((total, ff), F32),
                pltpu.VMEM((total, ff), F32),
                pltpu.VMEM((total // 2, ff), F32),
                pltpu.VMEM((total // 2, ff), F32),
                pltpu.VMEM((total, ff), BF16),
                pltpu.VMEM((line, 2, 2, tb, dc), BF16),
                pltpu.VMEM((rounds, line, 2, tb, half), BF16),
                pltpu.VMEM((rounds, line, 2, tb, half), BF16),
                pltpu.VMEM((rounds, line, tb, half), BF16),
                pltpu.VMEM((rounds, line, tb, half), BF16),
                pltpu.VMEM((rounds, line, tb, half), BF16),
                pltpu.VMEM((rounds, line, tb, half), BF16),
                pltpu.VMEM((rounds, line, tb, 2 * half), BF16),
                pltpu.VMEM((rounds, line, tb, 2 * half), BF16),
                pltpu.VMEM((tb, dc), F32),
                pltpu.VMEM((2, tb, 128), F32),
                dma((3 * rounds,)),
                dma((2,)),
                dma((3,)),
                dma((rounds * line,)),
                dma((rounds * line,)),
                dma((rounds * line,)),
                dma((rounds * line,)),
                dma((rounds * line,)),
                dma((3,)),
                dma((tiles,)),
                dma((tiles,)),
                dma((tiles,)),
                dma((4 * rounds,)),
                dma((4 * rounds,)),
                dma((rounds * line,)),
                dma((rounds * line,)),
            ],
            compiler_params=pltpu.CompilerParams(
                collective_id=0, has_side_effects=True, vmem_limit_bytes=67_043_328
            ),
        )(tokens, norm_gain.reshape(1, dc), gate_weight, up_weight, down_weight)

    return jax.shard_map(
        step,
        mesh=mesh,
        in_specs=(P("row", "col"), P("col"), P("col", "row"), P("col", "row"), P("row", "col")),
        out_specs=P("row", "col"),
        check_vma=False,
    )
```

```python
import functools

import jax
import jax.numpy as jnp
from jax import lax
from jax.experimental import pallas as pl
from jax.experimental.pallas import tpu as pltpu
from jax.sharding import PartitionSpec as P

MESH = pl.DeviceIdType.MESH
D = 8192
F32 = jnp.float32
BF16 = jnp.bfloat16


def tile_of(width):
    return 256 if width % 256 == 0 else width


def kernel(line, rounds, lead, out_rounds, ahead, lag, tokens, gain, gate_hbm, up_hbm, down_hbm, out,
           wg, wu, wd, act, gacc, uacc, rg, ru, hid, part, xa, yb, ya, xb, sa, sb, vs, zin, own, sq,
           wsem, sqs, ag_send, ag_z, ag_x, ag_y, ag_xh, ag_yh, c_send, cg, cu, ch,
           rs_s, rs_r, rz_s, rz_r):
    tb, dc = tokens.shape
    ff = wg.shape[1]
    n = 4 * line
    total = n * tb
    wide = dc // rounds
    half = wide // 2
    me = lax.axis_index("row")
    c = lax.axis_index("col")
    l, j, i = me // 4, (me // 2) % 2, me % 2

    def row(a, b, d):
        return (a * 2 + b) * 2 + d

    x_id = {"row": row(l, j, 1 - i)}
    y_id = {"row": row(l, 1 - j, i)}
    p_id = {"col": 1 - c}

    def z_at(k):
        return lax.rem(l + k, line)

    def from_z(k):
        return lax.rem(l + line - k, line)

    def z_id(k):
        return {"row": row(z_at(k), j, i)}

    def remote(src, dst, ssem, rsem, dev):
        return pltpu.make_async_remote_copy(src_ref=src, dst_ref=dst, send_sem=ssem, recv_sem=rsem,
                                            device_id=dev, device_id_type=MESH)

    loads = []
    for r in range(rounds):
        rows = pl.ds(r * wide, wide)
        loads.append([pltpu.make_async_copy(gate_hbm.at[rows], wg.at[rows], wsem.at[3 * r]),
                      pltpu.make_async_copy(up_hbm.at[rows], wu.at[rows], wsem.at[3 * r + 1])])
    frows = ff // rounds
    downs = [pltpu.make_async_copy(down_hbm.at[pl.ds(r * frows, frows)], wd.at[pl.ds(r * frows, frows)],
                                   wsem.at[3 * r + 2]) for r in range(rounds)]
    queue = loads + [downs]

    def fetch(at):
        if at < len(queue):
            for d in queue[at]:
                d.start()

    fetch(0)
    fetch(1)

    barrier = pltpu.get_barrier_semaphore()
    friends = [x_id, y_id, p_id] + [z_id(k) for k in range(1, line)]
    for dev in friends:
        pl.semaphore_signal(barrier, inc=1, device_id=dev, device_id_type=MESH)

    widened = tokens[...].astype(F32)
    mine = jnp.sum(widened * widened, axis=1, keepdims=True)
    sq[0] = jnp.broadcast_to(mine, (tb, 128))
    pl.semaphore_wait(barrier, len(friends))
    swap = remote(sq.at[0], sq.at[1], sqs.at[0], sqs.at[1], p_id)
    swap.start()
    scaled = widened * gain[...]
    swap.wait()
    squares = mine + sq[1][:, :1]
    act[me] = (scaled / jnp.sqrt(squares / D + 1e-05)).astype(BF16)

    def cols(r):
        return pl.ds(r * wide, wide)

    def cols_a(r):
        return pl.ds(r * wide, half)

    def cols_b(r):
        return pl.ds(r * wide + half, half)

    def move(b, where, sem, ssem, dev):
        ref = act.at[b, :, where]
        return remote(ref, ref, ssem, sem, dev)

    def to_xy(r, k):
        b = row(from_z(k), j, i)
        move(b, cols(r), ag_x.at[r * line + k], ag_send.at[0], x_id).start()
        move(b, cols(r), ag_y.at[r * line + k], ag_send.at[1], y_id).start()

    for r in range(rounds):
        for k in range(1, line):
            move(me, cols(r), ag_z.at[r * line + k], ag_send.at[2], z_id(k)).start()
        to_xy(r, 0)

    def along_z(r, first, end):
        for k in range(first, end):
            move(row(from_z(k), j, i), cols(r), ag_z.at[r * line + k], ag_send.at[2], z_id(k)).wait_recv()
            to_xy(r, k)

    def across(r, first, end):
        for k in range(first, end):
            b = row(from_z(k), 1 - j, i)
            move(b, cols(r), ag_y.at[r * line + k], ag_send.at[1], y_id).wait_recv()
            move(b, cols_a(r), ag_xh.at[r * line + k], ag_send.at[0], x_id).start()
            b = row(from_z(k), j, 1 - i)
            move(b, cols(r), ag_x.at[r * line + k], ag_send.at[0], x_id).wait_recv()
            move(b, cols_b(r), ag_yh.at[r * line + k], ag_send.at[1], y_id).start()

    def last_arrivals(r):
        for k in range(line):
            b = row(from_z(k), 1 - j, 1 - i)
            move(b, cols_a(r), ag_xh.at[r * line + k], ag_send.at[0], x_id).wait_recv()
            move(b, cols_b(r), ag_yh.at[r * line + k], ag_send.at[1], y_id).wait_recv()

    tw = tile_of(ff)
    tiles = ff // tw
    mrows = total // 2

    def tile(t):
        return pl.ds(pl.multiple_of(t * tw, tw), tw) if tiles > 1 else pl.ds(0, tw)

    theirs = pl.ds(pl.multiple_of((1 - c) * mrows, mrows), mrows)
    ours = pl.ds(pl.multiple_of(c * mrows, mrows), mrows)
    mstep = min(total, 256)

    def swap_tile(t):
        return [remote(gacc.at[theirs, tile(t)], rg.at[:, tile(t)], c_send.at[0], cg.at[t], p_id),
                remote(uacc.at[theirs, tile(t)], ru.at[:, tile(t)], c_send.at[1], cu.at[t], p_id)]

    def project(r):
        for d in loads[r]:
            d.wait()
        fetch(r + 2)
        wrows = pl.ds(r * wide, wide)
        last = r == rounds - 1

        def body(t, carry):
            for m in range(0, total, mstep):
                left = act[m // tb:(m + mstep) // tb, :, r * wide:(r + 1) * wide].reshape(mstep, wide)
                at = pl.ds(m, mstep)
                for w, acc in ((wg, gacc), (wu, uacc)):
                    value = jnp.dot(left, w[wrows, tile(t)], preferred_element_type=F32)
                    if r > 0:
                        value = acc[at, tile(t)] + value
                    acc[at, tile(t)] = value
            if last:
                @pl.when(t > 0)
                def _():
                    for d in swap_tile(t - 1):
                        d.start()
            return carry

        lax.fori_loop(0, tiles, body, 0)
        if last:
            for d in swap_tile(tiles - 1):
                d.start()

    along_z(0, 1, 2)
    for r in range(rounds):
        across(r, 0, 1)
    along_z(0, 2, line)
    for r in range(1, min(lead, rounds)):
        along_z(r, 1, line)
    across(0, 1, line)
    for r in range(rounds):
        if r + lead < rounds:
            along_z(r + lead, 1, line)
        if r + 1 < rounds:
            across(r + 1, 1, line)
        last_arrivals(r)
        project(r)

    def hid_tile(t):
        ref = hid.at[ours, tile(t)]
        return remote(ref, ref, c_send.at[2], ch.at[t], p_id)

    def gated(t, carry):
        for d in swap_tile(t):
            d.wait_recv()
        g = gacc[ours, tile(t)] + rg[:, tile(t)]
        u = uacc[ours, tile(t)] + ru[:, tile(t)]
        hid[ours, tile(t)] = (g / (1.0 + jnp.exp(-g)) * u).astype(BF16)

        @pl.when(t > 0)
        def _():
            hid_tile(t - 1).start()
        return carry

    lax.fori_loop(0, tiles, gated, 0)
    hid_tile(tiles - 1).start()
    for d in downs:
        d.wait()
    for t in range(tiles):
        ref = hid.at[theirs, tile(t)]
        remote(ref, ref, c_send.at[2], ch.at[t], p_id).wait_recv()

    def reduce_all(rounds):
        wide = dc // rounds
        half = wide // 2
        ow = tile_of(wide)
        oblocks = mstep // (4 * tb)

        def down(r):
            def body(t, carry):
                at = pl.ds(pl.multiple_of(r * wide + t * ow, ow), ow)
                for m in range(0, total, mstep):
                    value = jnp.dot(hid[pl.ds(m, mstep), :], wd[:, at], preferred_element_type=F32)
                    first = m // (4 * tb)
                    part[first:first + oblocks, :, :, :, at] = value.astype(BF16).reshape(oblocks, 2, 2, tb, ow)
                return carry

            lax.fori_loop(0, wide // ow, body, 0)

        def cols(r):
            return pl.ds(r * wide, wide)

        def cols_a(r):
            return pl.ds(r * wide, half)

        def cols_b(r):
            return pl.ds(r * wide + half, half)

        def first_x(r):
            return remote(part.at[:, :, 1 - i, :, cols_a(r)], xa.at[r], rs_s.at[4 * r], rs_r.at[4 * r], x_id)

        def first_y(r):
            return remote(part.at[:, 1 - j, :, :, cols_b(r)], yb.at[r], rs_s.at[4 * r + 1], rs_r.at[4 * r + 1], y_id)

        def second_y(r):
            return remote(sa.at[r], ya.at[r], rs_s.at[4 * r + 2], rs_r.at[4 * r + 2], y_id)

        def second_x(r):
            return remote(sb.at[r], xb.at[r], rs_s.at[4 * r + 3], rs_r.at[4 * r + 3], x_id)

        def third(r, k):
            return remote(vs.at[r, z_at(k)], zin.at[r, k], rz_s.at[r * line + k], rz_r.at[r * line + k], z_id(k))

        def s1(r):
            first_x(r).start()
            first_y(r).start()

        def s2(r):
            first_x(r).wait_recv()
            sa[r] = (part[:, 1 - j, i, :, cols_a(r)].astype(F32) + xa[r, :, 1 - j].astype(F32)).astype(BF16)
            second_y(r).start()
            first_y(r).wait_recv()
            sb[r] = (part[:, j, 1 - i, :, cols_b(r)].astype(F32) + yb[r, :, 1 - i].astype(F32)).astype(BF16)
            second_x(r).start()

        def s3(r):
            second_y(r).wait_recv()
            second_x(r).wait_recv()
            for where, near, far, lo in ((cols_a(r), xa, ya, 0), (cols_b(r), yb, xb, half)):
                mid = j if lo == 0 else i
                vs[r, :, :, lo:lo + half] = (part[:, j, i, :, where].astype(F32) + near[r, :, mid].astype(F32)
                                             + far[r].astype(F32)).astype(BF16)
                own[:, where] = (part[l, j, i, :, where].astype(F32) + near[r, l, mid].astype(F32)
                                 + far[r, l].astype(F32))
            for k in range(1, line):
                third(r, k).start()

        def s4(r):
            value = own[:, cols(r)]
            for k in range(1, line):
                third(r, k).wait_recv()
                value = value + zin[r, k].astype(F32)
            out[:, cols(r)] = value.astype(BF16)

        for r in range(rounds):
            down(r)
            if r < ahead:
                s1(r)
        for r in range(rounds + lag):
            if r < rounds:
                s2(r)
                if r + ahead < rounds:
                    s1(r + ahead)
            if r >= lag:
                s3(r - lag)
        for r in range(rounds):
            s4(r)
        for r in range(rounds):
            for make in (first_x, first_y, second_x, second_y):
                make(r).wait_send()
            for k in range(1, line):
                third(r, k).wait_send()

    reduce_all(out_rounds)

    for s, count in ((0, 3 * line // 2), (1, 3 * line // 2), (2, line - 1)):
        ref = act.at[pl.ds(0, count)]
        remote(ref, ref, ag_send.at[s], ag_z.at[0], x_id).wait_send()
    remote(rg, rg, c_send.at[0], cg.at[0], p_id).wait_send()
    remote(ru, ru, c_send.at[1], cu.at[0], p_id).wait_send()
    ref = hid.at[pl.ds(0, mrows)]
    remote(ref, ref, c_send.at[2], ch.at[0], p_id).wait_send()


def solution(mesh):
    n = mesh.shape["row"]
    line = n // 4

    def step(tokens, norm_gain, gate_weight, up_weight, down_weight):
        tb, dc = tokens.shape
        ff = gate_weight.shape[1]
        total = n * tb
        rounds, lead = 4, 2
        out_rounds, ahead, lag = 4, 2, 1
        half = dc // out_rounds // 2
        tiles = ff // tile_of(ff)
        dma = pltpu.SemaphoreType.DMA
        vmem = pl.BlockSpec(memory_space=pltpu.VMEM)
        hbm = pl.BlockSpec(memory_space=pl.ANY)
        return pl.pallas_call(
            functools.partial(kernel, line, rounds, lead, out_rounds, ahead, lag),
            out_shape=jax.ShapeDtypeStruct((tb, dc), BF16),
            in_specs=[vmem, vmem, hbm, hbm, hbm],
            out_specs=vmem,
            scratch_shapes=[
                pltpu.VMEM((dc, ff), BF16),
                pltpu.VMEM((dc, ff), BF16),
                pltpu.VMEM((ff, dc), BF16),
                pltpu.VMEM((n, tb, dc), BF16),
                pltpu.VMEM((total, ff), F32),
                pltpu.VMEM((total, ff), F32),
                pltpu.VMEM((total // 2, ff), F32),
                pltpu.VMEM((total // 2, ff), F32),
                pltpu.VMEM((total, ff), BF16),
                pltpu.VMEM((line, 2, 2, tb, dc), BF16),
                pltpu.VMEM((out_rounds, line, 2, tb, half), BF16),
                pltpu.VMEM((out_rounds, line, 2, tb, half), BF16),
                pltpu.VMEM((out_rounds, line, tb, half), BF16),
                pltpu.VMEM((out_rounds, line, tb, half), BF16),
                pltpu.VMEM((out_rounds, line, tb, half), BF16),
                pltpu.VMEM((out_rounds, line, tb, half), BF16),
                pltpu.VMEM((out_rounds, line, tb, 2 * half), BF16),
                pltpu.VMEM((out_rounds, line, tb, 2 * half), BF16),
                pltpu.VMEM((tb, dc), F32),
                pltpu.VMEM((2, tb, 128), F32),
                dma((3 * rounds,)),
                dma((2,)),
                dma((3,)),
                dma((rounds * line,)),
                dma((rounds * line,)),
                dma((rounds * line,)),
                dma((rounds * line,)),
                dma((rounds * line,)),
                dma((3,)),
                dma((tiles,)),
                dma((tiles,)),
                dma((tiles,)),
                dma((4 * out_rounds,)),
                dma((4 * out_rounds,)),
                dma((out_rounds * line,)),
                dma((out_rounds * line,)),
            ],
            compiler_params=pltpu.CompilerParams(
                collective_id=0, has_side_effects=True, vmem_limit_bytes=67_043_328
            ),
        )(tokens, norm_gain.reshape(1, dc), gate_weight, up_weight, down_weight)

    return jax.shard_map(
        step,
        mesh=mesh,
        in_specs=(P("row", "col"), P("col"), P("col", "row"), P("col", "row"), P("row", "col")),
        out_specs=P("row", "col"),
        check_vma=False,
    )
```

```python
import functools

import jax
import jax.numpy as jnp
from jax import lax
from jax.experimental import pallas as pl
from jax.experimental.pallas import tpu as pltpu
from jax.sharding import PartitionSpec as P

MESH = pl.DeviceIdType.MESH
D = 8192
F32 = jnp.float32
BF16 = jnp.bfloat16


def tile_of(width):
    return 256 if width % 256 == 0 else width


def kernel(line, rounds, lead, out_rounds, ahead, lag, tokens, gain, gate_hbm, up_hbm, down_hbm, out,
           wg, wu, wd, act, gacc, uacc, rg, ru, hid, part, xa, yb, ya, xb, sa, sb, vs, zin, own, sq,
           wsem, sqs, ag_send, ag_z, ag_x, ag_y, ag_xh, ag_yh, c_send, cg, cu, ch,
           rs_s, rs_r, rz_s, rz_r):
    tb, dc = tokens.shape
    ff = wg.shape[1]
    n = 4 * line
    total = n * tb
    wide = dc // rounds
    half = wide // 2
    me = lax.axis_index("row")
    c = lax.axis_index("col")
    l, j, i = me // 4, (me // 2) % 2, me % 2

    def row(a, b, d):
        return (a * 2 + b) * 2 + d

    x_id = {"row": row(l, j, 1 - i)}
    y_id = {"row": row(l, 1 - j, i)}
    p_id = {"col": 1 - c}

    def z_at(k):
        return lax.rem(l + k, line)

    def from_z(k):
        return lax.rem(l + line - k, line)

    def z_id(k):
        return {"row": row(z_at(k), j, i)}

    def remote(src, dst, ssem, rsem, dev):
        return pltpu.make_async_remote_copy(src_ref=src, dst_ref=dst, send_sem=ssem, recv_sem=rsem,
                                            device_id=dev, device_id_type=MESH)

    loads = []
    for r in range(rounds):
        rows = pl.ds(r * wide, wide)
        loads.append([pltpu.make_async_copy(gate_hbm.at[rows], wg.at[rows], wsem.at[3 * r]),
                      pltpu.make_async_copy(up_hbm.at[rows], wu.at[rows], wsem.at[3 * r + 1])])
    frows = ff // rounds
    downs = [pltpu.make_async_copy(down_hbm.at[pl.ds(r * frows, frows)], wd.at[pl.ds(r * frows, frows)],
                                   wsem.at[3 * r + 2]) for r in range(rounds)]
    queue = loads + [downs]

    def fetch(at):
        if at < len(queue):
            for d in queue[at]:
                d.start()

    fetch(0)
    fetch(1)

    barrier = pltpu.get_barrier_semaphore()
    friends = [x_id, y_id, p_id] + [z_id(k) for k in range(1, line)]
    for dev in friends:
        pl.semaphore_signal(barrier, inc=1, device_id=dev, device_id_type=MESH)

    widened = tokens[...].astype(F32)
    mine = jnp.sum(widened * widened, axis=1, keepdims=True)
    sq[0] = jnp.broadcast_to(mine, (tb, 128))
    pl.semaphore_wait(barrier, len(friends))
    swap = remote(sq.at[0], sq.at[1], sqs.at[0], sqs.at[1], p_id)
    swap.start()
    scaled = widened * gain[...]
    swap.wait()
    squares = mine + sq[1][:, :1]
    act[me] = (scaled / jnp.sqrt(squares / D + 1e-05)).astype(BF16)

    def cols(r):
        return pl.ds(r * wide, wide)

    def cols_a(r):
        return pl.ds(r * wide, half)

    def cols_b(r):
        return pl.ds(r * wide + half, half)

    def move(b, where, sem, ssem, dev):
        ref = act.at[b, :, where]
        return remote(ref, ref, ssem, sem, dev)

    def to_xy(r, k):
        b = row(from_z(k), j, i)
        move(b, cols(r), ag_x.at[r * line + k], ag_send.at[0], x_id).start()
        move(b, cols(r), ag_y.at[r * line + k], ag_send.at[1], y_id).start()

    for r in range(rounds):
        for k in range(1, line):
            move(me, cols(r), ag_z.at[r * line + k], ag_send.at[2], z_id(k)).start()
        to_xy(r, 0)

    def along_z(r, first, end):
        for k in range(first, end):
            move(row(from_z(k), j, i), cols(r), ag_z.at[r * line + k], ag_send.at[2], z_id(k)).wait_recv()
            to_xy(r, k)

    def across(r, first, end):
        for k in range(first, end):
            b = row(from_z(k), 1 - j, i)
            move(b, cols(r), ag_y.at[r * line + k], ag_send.at[1], y_id).wait_recv()
            move(b, cols_a(r), ag_xh.at[r * line + k], ag_send.at[0], x_id).start()
            b = row(from_z(k), j, 1 - i)
            move(b, cols(r), ag_x.at[r * line + k], ag_send.at[0], x_id).wait_recv()
            move(b, cols_b(r), ag_yh.at[r * line + k], ag_send.at[1], y_id).start()

    def last_arrivals(r):
        for k in range(line):
            b = row(from_z(k), 1 - j, 1 - i)
            move(b, cols_a(r), ag_xh.at[r * line + k], ag_send.at[0], x_id).wait_recv()
            move(b, cols_b(r), ag_yh.at[r * line + k], ag_send.at[1], y_id).wait_recv()

    tw = tile_of(ff)
    tiles = ff // tw
    mrows = total // 2

    def tile(t):
        return pl.ds(pl.multiple_of(t * tw, tw), tw) if tiles > 1 else pl.ds(0, tw)

    theirs = pl.ds(pl.multiple_of((1 - c) * mrows, mrows), mrows)
    ours = pl.ds(pl.multiple_of(c * mrows, mrows), mrows)
    mstep = min(total, 256)

    def swap_tile(t):
        return [remote(gacc.at[theirs, tile(t)], rg.at[:, tile(t)], c_send.at[0], cg.at[t], p_id),
                remote(uacc.at[theirs, tile(t)], ru.at[:, tile(t)], c_send.at[1], cu.at[t], p_id)]

    def project(r):
        for d in loads[r]:
            d.wait()
        fetch(r + 2)
        wrows = pl.ds(r * wide, wide)
        last = r == rounds - 1

        def body(t, carry):
            for m in range(0, total, mstep):
                left = act[m // tb:(m + mstep) // tb, :, r * wide:(r + 1) * wide].reshape(mstep, wide)
                at = pl.ds(m, mstep)
                for w, acc in ((wg, gacc), (wu, uacc)):
                    value = jnp.dot(left, w[wrows, tile(t)], preferred_element_type=F32)
                    if r > 0:
                        value = acc[at, tile(t)] + value
                    acc[at, tile(t)] = value
            if last:
                @pl.when(t > 0)
                def _():
                    for d in swap_tile(t - 1):
                        d.start()
            return carry

        lax.fori_loop(0, tiles, body, 0)
        if last:
            for d in swap_tile(tiles - 1):
                d.start()

    along_z(0, 1, 2)
    for r in range(rounds):
        across(r, 0, 1)
    along_z(0, 2, line)
    for r in range(1, min(lead, rounds)):
        along_z(r, 1, line)
    across(0, 1, line)
    for r in range(rounds):
        if r + lead < rounds:
            along_z(r + lead, 1, line)
        if r + 1 < rounds:
            across(r + 1, 1, line)
        last_arrivals(r)
        project(r)

    def hid_tile(t):
        ref = hid.at[ours, tile(t)]
        return remote(ref, ref, c_send.at[2], ch.at[t], p_id)

    def gated(t, carry):
        for d in swap_tile(t):
            d.wait_recv()
        g = gacc[ours, tile(t)] + rg[:, tile(t)]
        u = uacc[ours, tile(t)] + ru[:, tile(t)]
        hid[ours, tile(t)] = (g / (1.0 + jnp.exp(-g)) * u).astype(BF16)

        @pl.when(t > 0)
        def _():
            hid_tile(t - 1).start()
        return carry

    lax.fori_loop(0, tiles, gated, 0)
    hid_tile(tiles - 1).start()
    for d in downs:
        d.wait()
    for t in range(tiles):
        ref = hid.at[theirs, tile(t)]
        remote(ref, ref, c_send.at[2], ch.at[t], p_id).wait_recv()

    def reduce_all(rounds):
        wide = dc // rounds
        half = wide // 2
        ow = tile_of(half)
        oblocks = mstep // (4 * tb)

        def down(r, begin, end):
            def body(t, carry):
                at = pl.ds(pl.multiple_of(r * wide + t * ow, ow), ow)
                for m in range(0, total, mstep):
                    value = jnp.dot(hid[pl.ds(m, mstep), :], wd[:, at], preferred_element_type=F32)
                    first = m // (4 * tb)
                    part[first:first + oblocks, :, :, :, at] = value.astype(BF16).reshape(oblocks, 2, 2, tb, ow)
                return carry

            lax.fori_loop(begin, end, body, 0)

        def cols(r):
            return pl.ds(r * wide, wide)

        def cols_a(r):
            return pl.ds(r * wide, half)

        def cols_b(r):
            return pl.ds(r * wide + half, half)

        def first_x(r):
            return remote(part.at[:, :, 1 - i, :, cols_a(r)], xa.at[r], rs_s.at[4 * r], rs_r.at[4 * r], x_id)

        def first_y(r):
            return remote(part.at[:, 1 - j, :, :, cols_b(r)], yb.at[r], rs_s.at[4 * r + 1], rs_r.at[4 * r + 1], y_id)

        def second_y(r):
            return remote(sa.at[r], ya.at[r], rs_s.at[4 * r + 2], rs_r.at[4 * r + 2], y_id)

        def second_x(r):
            return remote(sb.at[r], xb.at[r], rs_s.at[4 * r + 3], rs_r.at[4 * r + 3], x_id)

        def third(r, k):
            return remote(vs.at[r, z_at(k)], zin.at[r, k], rz_s.at[r * line + k], rz_r.at[r * line + k], z_id(k))

        def s1(r):
            first_x(r).start()
            first_y(r).start()

        def s2(r):
            first_x(r).wait_recv()
            sa[r] = (part[:, 1 - j, i, :, cols_a(r)].astype(F32) + xa[r, :, 1 - j].astype(F32)).astype(BF16)
            second_y(r).start()
            first_y(r).wait_recv()
            sb[r] = (part[:, j, 1 - i, :, cols_b(r)].astype(F32) + yb[r, :, 1 - i].astype(F32)).astype(BF16)
            second_x(r).start()

        def s3(r):
            second_y(r).wait_recv()
            second_x(r).wait_recv()
            for where, near, far, lo in ((cols_a(r), xa, ya, 0), (cols_b(r), yb, xb, half)):
                mid = j if lo == 0 else i
                vs[r, :, :, lo:lo + half] = (part[:, j, i, :, where].astype(F32) + near[r, :, mid].astype(F32)
                                             + far[r].astype(F32)).astype(BF16)
                own[:, where] = (part[l, j, i, :, where].astype(F32) + near[r, l, mid].astype(F32)
                                 + far[r, l].astype(F32))
            for k in range(1, line):
                third(r, k).start()

        def s4(r):
            value = own[:, cols(r)]
            for k in range(1, line):
                third(r, k).wait_recv()
                value = value + zin[r, k].astype(F32)
            out[:, cols(r)] = value.astype(BF16)

        for r in range(rounds):
            down(r, 0, half // ow)
            if r < ahead:
                first_x(r).start()
            down(r, half // ow, wide // ow)
            if r < ahead:
                first_y(r).start()
        for r in range(rounds + lag):
            if r < rounds:
                s2(r)
                if r + ahead < rounds:
                    s1(r + ahead)
            if r >= lag:
                s3(r - lag)
        for r in range(rounds):
            s4(r)
        for r in range(rounds):
            for make in (first_x, first_y, second_x, second_y):
                make(r).wait_send()
            for k in range(1, line):
                third(r, k).wait_send()

    reduce_all(out_rounds)

    for s, count in ((0, 3 * line // 2), (1, 3 * line // 2), (2, line - 1)):
        ref = act.at[pl.ds(0, count)]
        remote(ref, ref, ag_send.at[s], ag_z.at[0], x_id).wait_send()
    remote(rg, rg, c_send.at[0], cg.at[0], p_id).wait_send()
    remote(ru, ru, c_send.at[1], cu.at[0], p_id).wait_send()
    ref = hid.at[pl.ds(0, mrows)]
    remote(ref, ref, c_send.at[2], ch.at[0], p_id).wait_send()


def solution(mesh):
    n = mesh.shape["row"]
    line = n // 4

    def step(tokens, norm_gain, gate_weight, up_weight, down_weight):
        tb, dc = tokens.shape
        ff = gate_weight.shape[1]
        total = n * tb
        rounds, lead = 4, 2
        out_rounds, ahead, lag = 4, 2, 1
        half = dc // out_rounds // 2
        tiles = ff // tile_of(ff)
        dma = pltpu.SemaphoreType.DMA
        vmem = pl.BlockSpec(memory_space=pltpu.VMEM)
        hbm = pl.BlockSpec(memory_space=pl.ANY)
        return pl.pallas_call(
            functools.partial(kernel, line, rounds, lead, out_rounds, ahead, lag),
            out_shape=jax.ShapeDtypeStruct((tb, dc), BF16),
            in_specs=[vmem, vmem, hbm, hbm, hbm],
            out_specs=vmem,
            scratch_shapes=[
                pltpu.VMEM((dc, ff), BF16),
                pltpu.VMEM((dc, ff), BF16),
                pltpu.VMEM((ff, dc), BF16),
                pltpu.VMEM((n, tb, dc), BF16),
                pltpu.VMEM((total, ff), F32),
                pltpu.VMEM((total, ff), F32),
                pltpu.VMEM((total // 2, ff), F32),
                pltpu.VMEM((total // 2, ff), F32),
                pltpu.VMEM((total, ff), BF16),
                pltpu.VMEM((line, 2, 2, tb, dc), BF16),
                pltpu.VMEM((out_rounds, line, 2, tb, half), BF16),
                pltpu.VMEM((out_rounds, line, 2, tb, half), BF16),
                pltpu.VMEM((out_rounds, line, tb, half), BF16),
                pltpu.VMEM((out_rounds, line, tb, half), BF16),
                pltpu.VMEM((out_rounds, line, tb, half), BF16),
                pltpu.VMEM((out_rounds, line, tb, half), BF16),
                pltpu.VMEM((out_rounds, line, tb, 2 * half), BF16),
                pltpu.VMEM((out_rounds, line, tb, 2 * half), BF16),
                pltpu.VMEM((tb, dc), F32),
                pltpu.VMEM((2, tb, 128), F32),
                dma((3 * rounds,)),
                dma((2,)),
                dma((3,)),
                dma((rounds * line,)),
                dma((rounds * line,)),
                dma((rounds * line,)),
                dma((rounds * line,)),
                dma((rounds * line,)),
                dma((3,)),
                dma((tiles,)),
                dma((tiles,)),
                dma((tiles,)),
                dma((4 * out_rounds,)),
                dma((4 * out_rounds,)),
                dma((out_rounds * line,)),
                dma((out_rounds * line,)),
            ],
            compiler_params=pltpu.CompilerParams(
                collective_id=0, has_side_effects=True, vmem_limit_bytes=67_043_328
            ),
        )(tokens, norm_gain.reshape(1, dc), gate_weight, up_weight, down_weight)

    return jax.shard_map(
        step,
        mesh=mesh,
        in_specs=(P("row", "col"), P("col"), P("col", "row"), P("col", "row"), P("row", "col")),
        out_specs=P("row", "col"),
        check_vma=False,
    )
```
